32 devices in a mesh: gz: 4 (over x, core), gx: 4 (over z), gy: 2 (over y).
Axes of the slice: x: 2, y: 2, z: 4, core: 2. Of those that a mesh axis runs over, the one named last changes fastest.
Arguments:
- offsets: float32 [3, 4, 8, 8, 128], P(None, 'gz', 'gx', 'gy'), may hold values from 0 to 10
- type_ids: int32 [4, 8, 8, 128], P('gz', 'gx', 'gy'), may hold values from 0 to 2
- occupied: int32 [4, 8, 8, 128], P('gz', 'gx', 'gy'), may hold values from 0 to 1, as said below
- prior_charges: float32 [2, 4, 8, 8, 128], P(None, 'gz', 'gx', 'gy'), may hold values from -0.6 to 0.6
- electronegativity: float32 [3], replicated, may hold values from 2 to 10
- hardness: float32 [3], replicated, may hold values from 4 to 12
- shielding: float32 [3], replicated, may hold values from 0.5 to 1.2
Outputs:
- charges: float32 [4, 8, 8, 128], P('gz', 'gx', 'gy')
- residuals: float32 [2, 4, 8, 8, 128], P(None, 'gz', 'gx', 'gy')
The draws below stay inside these ranges and needn't reach their ends.
Inputs may be any that keep to these rules, and one draw needn't show every extreme that they name: `occupied`: 1 marks a slot that holds an atom, 0 a padding slot.
All inputs are finite; a program needn't handle non-finite values.
Results may differ from the reference program's by a relative error of at most 0.00021.
Values sent between devices are 32-bit elements; how exact they have to be, the bound alone decides.
A program may use at most 128 MiB of HBM per device.

```python
import jax
import jax.numpy as jnp
from jax import lax

SLOTS = 128
ITERS = 4
NTYPES = 3
NCZ = 4
NCX = 8
NCY = 8


def draw_occupied(key, part):
    shape = (NCZ, NCX, NCY, SLOTS)
    layer = jnp.arange(NCZ, dtype=jnp.int32)[:, None, None, None]
    threshold = 250 + 700 * layer // max(NCZ - 1, 1)
    rolled = jax.random.randint(jax.random.fold_in(key, 17), shape, 0, 1000)
    return (rolled < threshold).astype(jnp.int32)


def place_ends(entries, rng, smallest, high):
    place = [jax.random.randint(jax.random.fold_in(rng, axis), (), 0, length) for axis, length in enumerate(entries.shape)]
    longest = entries.shape.index(max(entries.shape))
    neighbour = place[:longest] + [(place[longest] + 1) % entries.shape[longest]] + place[longest + 1:]
    return entries.at[tuple(place)].set(smallest).at[tuple(neighbour)].set(high)


def levels(stream_key, shape, shards, least, top_value):
    def one(dim, blocks):
        heights = jax.random.uniform(jax.random.fold_in(jax.random.fold_in(stream_key, 6), dim), (blocks,), jnp.float32, least / len(shards), top_value / len(shards))
        return jnp.repeat(jnp.exp(heights), shape[dim] // blocks).reshape((-1,) + (1,) * (len(shape) - dim - 1))

    gain = one(*shards[0])
    for cut in shards[1:]:
        gain = gain * one(*cut)
    return gain


def bell_draw(stream_key, shape, deviation, limit, split=(), kind=jnp.bfloat16):
    result = jax.random.normal(stream_key, shape, jnp.float32) * deviation
    if len(split) > 0:
        result = levels(stream_key, shape, split, -0.22, 0.18) * result
    return jnp.clip(result, min=-limit, max=limit).astype(kind)


def setup_inputs(seed: int = 0) -> dict:
    streams_of = jax.random.split(jax.random.key(seed), 8)
    offsets = jnp.clip(10.0 * jax.random.uniform(streams_of[0], (3, NCZ, NCX, NCY, SLOTS), jnp.float32) ** levels(streams_of[0], (3, NCZ, NCX, NCY, SLOTS), ((1, 4), (2, 4), (3, 2)), -0.2, 0.2), 0.0, 10.0)
    type_ids = place_ends(jax.random.randint(streams_of[1], (NCZ, NCX, NCY, SLOTS), 0, NTYPES), jax.random.fold_in(streams_of[1], 1), 0, NTYPES - 1).astype(jnp.int32)
    occupied = draw_occupied(jax.random.fold_in(streams_of[7], 71), 0)
    prior_charges = bell_draw(streams_of[3], (2, NCZ, NCX, NCY, SLOTS), 0.1, 0.6, ((1, 4), (2, 4), (3, 2)), jnp.float32)
    electronegativity = jnp.clip(jax.random.uniform(streams_of[4], (NTYPES,), jnp.float32, 2.0, 10.0), 2.0, 10.0)
    hardness = jnp.clip(jax.random.uniform(streams_of[5], (NTYPES,), jnp.float32, 4.0, 12.0), 4.0, 12.0)
    shielding = jnp.clip(jax.random.uniform(streams_of[6], (NTYPES,), jnp.float32, 0.5, 1.2), 0.5, 1.2)
    return {"offsets": offsets, "type_ids": type_ids, "occupied": occupied, "prior_charges": prior_charges, "electronegativity": electronegativity, "hardness": hardness, "shielding": shielding}


coulomb_factor = 14.4
cell_edge = 10.0

def per_atom(values_table, type_ids):
    summed = jnp.zeros(type_ids.shape, jnp.float32)
    for species in range(values_table.shape[0]):
        summed = summed + jnp.where(type_ids == species, values_table[species], 0.0)
    return summed

def pair_sum(local_geo, beside, remote, shift):
    delta_z = shift[0] * cell_edge + beside[0][..., None, :] - local_geo[0][..., :, None]
    delta_x = shift[1] * cell_edge + beside[1][..., None, :] - local_geo[1][..., :, None]
    delta_y = shift[2] * cell_edge + beside[2][..., None, :] - local_geo[2][..., :, None]
    squared = delta_z * delta_z + delta_x * delta_x + delta_y * delta_y
    fraction = jnp.sqrt(squared) / cell_edge
    reach = jnp.maximum(1.0 - fraction, 0.0)
    reach = reach * reach
    taper = reach * reach * (4.0 * fraction + 1.0)
    kernel = coulomb_factor * lax.rsqrt(squared + local_geo[3][..., :, None] + beside[3][..., None, :]) * taper
    return lax.optimization_barrier(jnp.sum(kernel[None] * remote[..., None, :], axis=-1))

def couple(geometry, field):
    geo_padded = jnp.pad(geometry, ((0, 0), (1, 1), (0, 0), (0, 0), (0, 0)))
    field_padded = jnp.pad(field, ((0, 0), (1, 1), (0, 0), (0, 0), (0, 0)))

    def z_plane(index_z):
        geo_slab = lax.dynamic_slice_in_dim(geo_padded, index_z, 3, 1)
        field_slab = lax.dynamic_slice_in_dim(field_padded, index_z, 3, 1)
        local_geo = geo_slab[:, 1]
        summed = jnp.zeros((field.shape[0],) + local_geo.shape[1:], jnp.float32)
        for off_z in range(3):
            for off_x in range(3):
                for off_y in range(3):
                    beside = jnp.roll(geo_slab[:, off_z], (1 - off_x, 1 - off_y), axis=(1, 2))
                    remote = jnp.roll(field_slab[:, off_z], (1 - off_x, 1 - off_y), axis=(1, 2))
                    summed = summed + pair_sum(local_geo, beside, remote, (off_z - 1, off_x - 1, off_y - 1))
        return summed
    planes = lax.map(z_plane, jnp.arange(NCZ, dtype=jnp.int32))
    return jnp.moveaxis(planes, 0, 1)

def inner_sum(left, right):
    return lax.optimization_barrier(jnp.sum(left * right, axis=(1, 2, 3, 4)))

def expand(scalars):
    return scalars[:, None, None, None, None]

def reference(offsets, type_ids, occupied, prior_charges, electronegativity, hardness, shielding):
    occupancy = occupied.astype(jnp.float32)
    stiffness = per_atom(hardness, type_ids)
    affinity = per_atom(electronegativity, type_ids)
    radius = per_atom(shielding, type_ids)
    geometry = jnp.concatenate([offsets, (radius * radius)[None]], axis=0)

    def operate(field):
        return occupancy[None] * (stiffness[None] * field + couple(geometry, field))
    rhs = jnp.stack([-affinity * occupancy, -occupancy])
    iterate = prior_charges * occupancy[None]
    residual = rhs - operate(iterate)
    direction = residual
    norm_now = inner_sum(residual, residual)
    for iteration in range(ITERS):
        image = operate(direction)
        step_size = norm_now / inner_sum(direction, image)
        iterate = iterate + expand(step_size) * direction
        residual = residual - expand(step_size) * image
        norm_next = inner_sum(residual, residual)
        direction = residual + expand(norm_next / norm_now) * direction
        norm_now = norm_next
    totals = lax.optimization_barrier(jnp.sum(iterate, axis=(1, 2, 3, 4)))
    charges = iterate[0] - totals[0] / totals[1] * iterate[1]
    return (charges, residual)
```

```python
import functools

import jax
import jax.numpy as jnp
from jax import lax
from jax.experimental import pallas as pl
from jax.experimental.pallas import tpu as pltpu
from jax.sharding import PartitionSpec as P

ITERS = 4
AXES = ("gz", "gx", "gy")
MESH = pl.DeviceIdType.MESH

coulomb_factor = 14.4
cell_edge = 10.0
CHUNK = 64


def kernel(
    sizes, dys,
    offsets, type_ids, occupied, prior, electro, hardness, shielding,
    charges, residuals,
    first, fields, pair, local, sums, parts, mine,
    send_sem, recv_sem, part_send, part_recv,
):
    nz, nx, ny = sizes
    cells_x, cells_y, slots = type_ids.shape[1:]
    rows = 2 * cells_y
    geo_rows = 4 * cells_y
    cells = cells_x * cells_y
    devices = nz * nx * ny
    me_z, me_x, me_y = (lax.axis_index(name) for name in AXES)

    at_x = [lax.rem(me_x + d, nx) for d in range(nx)]
    at_y = [lax.rem(me_y + d, ny) for d in range(ny)]

    def each_peer(action):
        def layer(dz, skip):
            z = lax.rem(me_z + dz, nz)
            for dx in range(nx):
                for dy in range(ny):
                    if not (skip and dx == 0 and dy == 0):
                        action((z, at_x[dx], at_y[dy]), (dz * nx + dx) * ny + dy - 1)

        layer(0, True)
        if nz <= 4:
            for dz in range(1, nz):
                layer(dz, False)
        else:
            pl.loop(1, nz)(lambda dz: layer(dz, False))

    barrier = pltpu.get_barrier_semaphore()
    each_peer(
        lambda peer, slot: pl.semaphore_signal(
            barrier, inc=1, device_id=peer, device_id_type=MESH
        )
    )

    def per_atom(table, ids):
        summed = jnp.zeros(ids.shape, jnp.float32)
        for species in range(table.shape[0]):
            summed = summed + jnp.where(ids == species, table[species], 0.0)
        return summed

    occ, stiff, rhs, x = [], [], [], []
    for i in range(cells_x):
        ids = type_ids[0, i]
        occ_i = occupied[0, i].astype(jnp.float32)
        radius = per_atom(shielding, ids) * (1.0 / cell_edge)
        for c in range(3):
            first[1, 0, i + 1, c * cells_y : (c + 1) * cells_y] = offsets[c, 0, i] * (
                1.0 / cell_edge
            )
        first[1, 0, i + 1, 3 * cells_y : geo_rows] = radius * radius
        stiff_i = per_atom(hardness, ids)
        affinity = per_atom(electro, ids)
        occ.append(jnp.concatenate([occ_i, occ_i], axis=0))
        stiff.append(jnp.concatenate([stiff_i, stiff_i], axis=0))
        rhs.append(jnp.concatenate([-affinity * occ_i, -occ_i], axis=0))
        start = jnp.concatenate([prior[0, 0, i] * occ_i, prior[1, 0, i] * occ_i], axis=0)
        x.append(start)
        first[1, 0, i + 1, geo_rows:] = start

    for edge, slot in ((0, 0), (nz - 1, 2)):

        @pl.when(me_z == edge)
        def _():
            first[slot] = jnp.zeros(first.shape[1:], jnp.float32)
            for k in range(ITERS):
                fields[k, slot] = jnp.zeros(fields.shape[2:], jnp.float32)

    messages = [
        (dz, dx, dy)
        for dz in (0, 1, -1)
        for dx in (0, 1, -1)
        for dy in dys
        if (dz, dx, dy) != (0, 0, 0)
    ]
    turn_x = {d: lax.rem(me_x + d + nx, nx) for d in (0, 1, -1)}
    turn_y = {d: lax.rem(me_y + d + ny, ny) for d in (0, 1, -1)}

    def copies(stage, buffer, action):
        for m, (dz, dx, dy) in enumerate(messages):
            source, target = {
                0: (pl.ds(1, cells_x), pl.ds(1, cells_x)),
                1: (pl.ds(cells_x, 1), pl.ds(0, 1)),
                -1: (pl.ds(1, 1), pl.ds(cells_x + 1, 1)),
            }[dx]
            copy = pltpu.make_async_remote_copy(
                src_ref=buffer.at[1, 0, source],
                dst_ref=buffer.at[1 - dz, dys.index(dy), target],
                send_sem=send_sem.at[stage, m],
                recv_sem=recv_sem.at[stage, m],
                device_id=(me_z + dz, turn_x[dx], turn_y[dy]),
                device_id_type=MESH,
            )
            action(copy, dz)

    def send(stage, buffer):
        def go(copy, dz):
            if dz == 0:
                copy.start()
            else:
                pl.when((me_z + dz >= 0) & (me_z + dz < nz))(copy.start)

        copies(stage, buffer, go)

    def receive(stage, buffer):
        def go(copy, dz):
            if dz == 0:
                copy.wait_recv()
            else:
                pl.when((me_z - dz >= 0) & (me_z - dz < nz))(copy.wait_recv)

        copies(stage, buffer, go)

    def sent(stage, buffer):
        def go(copy, dz):
            if dz == 0:
                copy.wait_send()
            else:
                pl.when((me_z + dz >= 0) & (me_z + dz < nz))(copy.wait_send)

        copies(stage, buffer, go)

    pl.semaphore_wait(barrier, devices - 1)
    send(0, first)

    shape = (slots, slots)
    eye = lax.broadcasted_iota(jnp.int32, shape, 0) == lax.broadcasted_iota(jnp.int32, shape, 1)

    @pl.loop(0, cells)
    def _(cell):
        i, j = cell // cells_y, cell % cells_y
        for c in range(4):
            row = first[1, 0, i + 1, pl.ds(c * cells_y + j, 1), :]
            column = jnp.sum(jnp.where(eye, row, 0.0), axis=1, keepdims=True)
            local[cell, c] = jnp.broadcast_to(column, shape)

    def beside(j, dy):
        y = j + dy
        if dy == 0:
            return 0, y
        if dy < 0:
            out = y < 0
            return jnp.where(out, 1, 0), jnp.where(out, y + cells_y, y)
        out = y >= cells_y
        return jnp.where(out, len(dys) - 1, 0), jnp.where(out, y - cells_y, y)

    def build():
        @pl.loop(0, cells)
        def _(cell):
            i, j = cell // cells_y, cell % cells_y
            where = [beside(j, dy) for dy in (-1, 0, 1)]

            @pl.loop(0, 9)
            def _(plane):
                dz, dx = plane // 3, plane % 3
                shift_z = (dz - 1).astype(jnp.float32)
                shift_x = (dx - 1).astype(jnp.float32)
                for k in range(3):
                    side, y = where[k]
                    tile = first.at[dz, side, i + dx]
                    bz = tile[pl.ds(y, 1), :] + shift_z
                    bx = tile[pl.ds(cells_y + y, 1), :] + shift_x
                    by = tile[pl.ds(2 * cells_y + y, 1), :] + (k - 1.0)
                    bs = tile[pl.ds(3 * cells_y + y, 1), :]
                    for part in range(slots // CHUNK):
                        span = pl.ds(part * CHUNK, CHUNK)
                        ez = bz - local[cell, 0, span]
                        ex = bx - local[cell, 1, span]
                        ey = by - local[cell, 2, span]
                        squared = ez * ez + ex * ex + ey * ey
                        fraction = squared * lax.rsqrt(jnp.maximum(squared, 1e-30))
                        reach = jnp.maximum(1.0 - fraction, 0.0)
                        reach = reach * reach
                        factor = coulomb_factor / cell_edge
                        taper = reach * reach * (4.0 * factor * fraction + factor)
                        pair[cell, plane * 3 + k, span] = taper * lax.rsqrt(
                            squared + (local[cell, 3, span] + bs)
                        )

    def operate(buffer, base, field):
        @pl.loop(0, cells)
        def _(cell):
            i, j = cell // cells_y, cell % cells_y
            where = [beside(j, dy) for dy in (-1, 0, 1)]
            total = [jnp.zeros(shape, jnp.float32) for _ in range(2)]
            for dz in range(3):
                for dx in range(3):
                    for k in range(3):
                        side, y = where[k]
                        tile = buffer.at[dz, side, i + dx]
                        block = pair[cell, (dz * 3 + dx) * 3 + k]
                        for s in range(2):
                            total[s] = total[s] + block * tile[
                                pl.ds(base + s * cells_y + y, 1), :
                            ]
            for s in range(2):
                sums[i, s * cells_y + j] = total[s]

        out = []
        for i in range(cells_x):
            lines = []
            for row in range(rows):
                column = jnp.sum(sums[i, row], axis=1, keepdims=True)
                lines.append(jnp.sum(jnp.where(eye, column, 0.0), axis=0, keepdims=True))
            out.append(occ[i] * (stiff[i] * field[i] + jnp.concatenate(lines, axis=0)))
        return out

    tile_shape = (rows, slots)
    lane = lax.broadcasted_iota(jnp.int32, tile_shape, 1)
    second = lax.broadcasted_iota(jnp.int32, tile_shape, 0) >= cells_y
    slot_of = lane - jnp.where(second, 8, 0)

    def part_copy(stage, peer, slot):
        return pltpu.make_async_remote_copy(
            src_ref=mine.at[stage],
            dst_ref=parts.at[stage, slot],
            send_sem=part_send.at[stage],
            recv_sem=part_recv.at[stage],
            device_id=peer,
            device_id_type=MESH,
        )

    def start_sums(stage, quantities):
        packed = jnp.zeros(tile_shape, jnp.float32)
        for k, quantity in enumerate(quantities):
            column = jnp.sum(functools.reduce(jnp.add, quantity), axis=1, keepdims=True)
            packed = jnp.where(slot_of == k, column, packed)
        mine[stage] = jnp.sum(packed, axis=0, keepdims=True)
        each_peer(lambda peer, slot: part_copy(stage, peer, slot).start())

    def finish_sums(stage, count):
        everything = parts.at[stage]
        pltpu.make_async_copy(everything, everything, part_recv.at[stage]).wait()
        row = mine[stage] + jnp.sum(parts[stage], axis=0)
        pltpu.make_async_copy(everything, everything, part_send.at[stage]).wait()
        return [
            jnp.where(
                second,
                jnp.broadcast_to(row[:, 8 + k : 9 + k], tile_shape),
                jnp.broadcast_to(row[:, k : k + 1], tile_shape),
            )
            for k in range(count)
        ]

    span = range(cells_x)

    def exchange_and_operate(stage, field):
        buffer = fields.at[stage - 1]
        for i in span:
            buffer[1, 0, i + 1] = field[i]
        send(stage, buffer)
        receive(stage, buffer)
        out = operate(buffer, 0, field)
        sent(stage, buffer)
        return out

    receive(0, first)
    build()
    image = operate(first, geo_rows, x)
    sent(0, first)
    r = [rhs[i] - image[i] for i in span]
    w = exchange_and_operate(1, r)

    p = s = z = None
    for stage in range(ITERS):
        quantities = [[r[i] * r[i] for i in span], [w[i] * r[i] for i in span]]
        last = stage == ITERS - 1
        if last:
            quantities += [x, r, p]
        start_sums(stage, quantities)
        n = None if last else exchange_and_operate(stage + 2, w)
        found = finish_sums(stage, len(quantities))
        gamma, delta = found[:2]
        if stage == 0:
            beta = None
            alpha = gamma / delta
            p, s, z = r, w, n
        else:
            beta = gamma / gamma_before
            alpha = gamma / (delta - beta * gamma / alpha)
            p = [r[i] + beta * p[i] for i in span]
            s = [w[i] + beta * s[i] for i in span]
            if not last:
                z = [n[i] + beta * z[i] for i in span]
        gamma_before = gamma
        x = [x[i] + alpha * p[i] for i in span]
        r = [r[i] - alpha * s[i] for i in span]
        if not last:
            w = [w[i] - alpha * z[i] for i in span]
    totals = found[2] + alpha * (found[3] + beta * found[4])
    ratio = totals[:cells_y] / totals[cells_y:]
    for i in span:
        charges[0, i] = x[i][:cells_y] - ratio * x[i][cells_y:]
        residuals[0, 0, i] = r[i][:cells_y]
        residuals[1, 0, i] = r[i][cells_y:]


def per_device(sizes, *arrays):
    type_ids = arrays[1]
    cells_x, cells_y, slots = type_ids.shape[1:]
    cells = cells_x * cells_y
    rows = 2 * cells_y
    devices = sizes[0] * sizes[1] * sizes[2]
    dys = (0, 1) if sizes[2] == 2 else (0, 1, -1)
    messages = 9 * len(dys) - 1
    halo = (3, len(dys), cells_x + 2)
    vmem = pl.BlockSpec(memory_space=pltpu.VMEM)
    smem = pl.BlockSpec(memory_space=pltpu.SMEM)
    return pl.pallas_call(
        functools.partial(kernel, sizes, dys),
        out_shape=(
            jax.ShapeDtypeStruct(type_ids.shape, jnp.float32),
            jax.ShapeDtypeStruct((2,) + type_ids.shape, jnp.float32),
        ),
        in_specs=[vmem] * 4 + [smem] * 3,
        out_specs=(vmem, vmem),
        scratch_shapes=[
            pltpu.VMEM(halo + (6 * cells_y, slots), jnp.float32),
            pltpu.VMEM((ITERS,) + halo + (rows, slots), jnp.float32),
            pltpu.VMEM((cells, 27, slots, slots), jnp.float32),
            pltpu.VMEM((cells, 4, slots, slots), jnp.float32),
            pltpu.VMEM((cells_x, rows, slots, slots), jnp.float32),
            pltpu.VMEM((ITERS, devices - 1, 1, slots), jnp.float32),
            pltpu.VMEM((ITERS, 1, slots), jnp.float32),
            pltpu.SemaphoreType.DMA((ITERS + 1, messages)),
            pltpu.SemaphoreType.DMA((ITERS + 1, messages)),
            pltpu.SemaphoreType.DMA((ITERS,)),
            pltpu.SemaphoreType.DMA((ITERS,)),
        ],
        compiler_params=pltpu.CompilerParams(
            collective_id=0, has_side_effects=True, vmem_limit_bytes=48 * 1024 * 1024
        ),
    )(*arrays)


def solution(mesh):
    sizes = tuple(mesh.shape[name] for name in AXES)
    in_specs = (
        P(None, "gz", "gx", "gy", None),
        P("gz", "gx", "gy", None),
        P("gz", "gx", "gy", None),
        P(None, "gz", "gx", "gy", None),
        P(),
        P(),
        P(),
    )
    out_specs = (P("gz", "gx", "gy", None), P(None, "gz", "gx", "gy", None))
    return jax.shard_map(
        functools.partial(per_device, sizes),
        mesh=mesh,
        in_specs=in_specs,
        out_specs=out_specs,
        check_vma=False,
    )
```

```python
import functools

import jax
import jax.numpy as jnp
from jax import lax
from jax.experimental import pallas as pl
from jax.experimental.pallas import tpu as pltpu
from jax.sharding import PartitionSpec as P

ITERS = 4
AXES = ("gz", "gx", "gy")
MESH = pl.DeviceIdType.MESH

coulomb_factor = 14.4
cell_edge = 10.0
CHUNK = 64


def kernel(
    sizes, dys,
    offsets_in, type_ids_in, occupied_in, prior_in, electro_in, hardness_in, shielding_in,
    charges, residuals,
    offsets, type_ids, occupied, prior, electro, hardness, shielding,
    first, fields, first_edge, edges, pair, local, sums, parts, mine,
    in_sem, send_sem, recv_sem, part_send, part_recv,
):
    loads = [
        pltpu.make_async_copy(source, target, in_sem.at[k])
        for k, (source, target) in enumerate(
            zip(
                (offsets_in, type_ids_in, occupied_in, prior_in,
                 electro_in, hardness_in, shielding_in),
                (offsets, type_ids, occupied, prior, electro, hardness, shielding),
            )
        )
    ]
    for load in loads:
        load.start()
    nz, nx, ny = sizes
    cells_x, cells_y, slots = type_ids.shape[1:]
    rows = 2 * cells_y
    geo_rows = 4 * cells_y
    cells = cells_x * cells_y
    devices = nz * nx * ny
    sides = len(dys) - 1
    me_z, me_x, me_y = (lax.axis_index(name) for name in AXES)

    at_x = [lax.rem(me_x + d, nx) for d in range(nx)]
    at_y = [lax.rem(me_y + d, ny) for d in range(ny)]

    def each_peer(action):
        def layer(dz, skip):
            z = lax.rem(me_z + dz, nz)
            for dx in range(nx):
                for dy in range(ny):
                    if not (skip and dx == 0 and dy == 0):
                        action((z, at_x[dx], at_y[dy]), (dz * nx + dx) * ny + dy - 1)

        layer(0, True)
        if nz <= 4:
            for dz in range(1, nz):
                layer(dz, False)
        else:
            pl.loop(1, nz)(lambda dz: layer(dz, False))

    barrier = pltpu.get_barrier_semaphore()
    each_peer(
        lambda peer, slot: pl.semaphore_signal(
            barrier, inc=1, device_id=peer, device_id_type=MESH
        )
    )

    def per_atom(table, ids):
        summed = jnp.zeros(ids.shape, jnp.float32)
        for species in range(table.shape[0]):
            summed = summed + jnp.where(ids == species, table[species], 0.0)
        return summed

    for load in loads:
        load.wait()
    occ, stiff, rhs, x = [], [], [], []

    def ends(values):
        return [values[:1], values[cells_y - 1 : cells_y]]

    for i in range(cells_x):
        ids = type_ids[0, i]
        occ_i = occupied[0, i].astype(jnp.float32)
        radius = per_atom(shielding, ids) * (1.0 / cell_edge)
        geo = [offsets[c, 0, i] * (1.0 / cell_edge) for c in range(3)] + [radius * radius]
        first[1, i + 1, :geo_rows] = jnp.concatenate(geo, axis=0)
        stiff_i = per_atom(hardness, ids)
        affinity = per_atom(electro, ids)
        occ.append(jnp.concatenate([occ_i, occ_i], axis=0))
        stiff.append(jnp.concatenate([stiff_i, stiff_i], axis=0))
        rhs.append(jnp.concatenate([-affinity * occ_i, -occ_i], axis=0))
        start = jnp.concatenate([prior[0, 0, i] * occ_i, prior[1, 0, i] * occ_i], axis=0)
        x.append(start)
        first[1, i + 1, geo_rows : geo_rows + rows] = start
        pieces = geo + [start[:cells_y], start[cells_y:]]
        first_edge[i] = jnp.concatenate([end for v in pieces for end in ends(v)], axis=0)

    for edge, slot in ((0, 0), (nz - 1, 2)):

        @pl.when(me_z == edge)
        def _():
            first[slot] = jnp.zeros(first.shape[1:], jnp.float32)
            for k in range(ITERS):
                fields[k, slot] = jnp.zeros(fields.shape[2:], jnp.float32)

    messages = [
        (dz, dx, dy)
        for dz in (1, -1, 0)
        for dx in (1, -1, 0)
        for dy in reversed(dys)
        if (dz, dx, dy) != (0, 0, 0)
    ]
    turn_x = {d: lax.rem(me_x + d + nx, nx) for d in (0, 1, -1)}
    turn_y = {d: lax.rem(me_y + d + ny, ny) for d in (0, 1, -1)}

    def copies(stage, buffer, edge, own_rows, action, layers=(1, -1, 0)):
        edge_rows = edge.shape[1]
        for m, (dz, dx, dy) in enumerate(messages):
            if dz not in layers:
                continue
            source, target, count = {
                0: (0, 1, cells_x),
                1: (cells_x - 1, 0, 1),
                -1: (0, cells_x + 1, 1),
            }[dx]
            if dy == 0:
                src = buffer.at[1, pl.ds(source + 1, count), pl.ds(0, own_rows)]
                span = pl.ds(0, own_rows)
            else:
                src = edge.at[pl.ds(source, count)]
                span = pl.ds(own_rows + (dys.index(dy) - 1) * edge_rows, edge_rows)
            copy = pltpu.make_async_remote_copy(
                src_ref=src,
                dst_ref=buffer.at[1 - dz, pl.ds(target, count), span],
                send_sem=send_sem.at[stage, m],
                recv_sem=recv_sem.at[stage, m],
                device_id=(me_z + dz, turn_x[dx], turn_y[dy]),
                device_id_type=MESH,
            )
            action(copy, dz)

    def guarded(name, sign):
        def go(copy, dz):
            act = getattr(copy, name)
            if dz == 0:
                act()
            else:
                other = me_z + sign * dz
                pl.when((other >= 0) & (other < nz))(act)

        return go

    def send(*what):
        copies(*what, guarded("start", 1))

    def receive(*what, layers=(1, -1, 0)):
        copies(*what, guarded("wait_recv", -1), layers)

    def sent(*what):
        copies(*what, guarded("wait_send", 1))

    opening = (0, first, first_edge, geo_rows + rows)
    pl.semaphore_wait(barrier, devices - 1)
    send(*opening)

    shape = (slots, slots)
    eye = lax.broadcasted_iota(jnp.int32, shape, 0) == lax.broadcasted_iota(jnp.int32, shape, 1)

    @pl.loop(0, cells)
    def _(cell):
        i, j = cell // cells_y, cell % cells_y
        for c in range(4):
            row = first[1, i + 1, pl.ds(c * cells_y + j, 1), :]
            column = jnp.sum(jnp.where(eye, row, 0.0), axis=1, keepdims=True)
            local[cell, c] = jnp.broadcast_to(column, shape)

    def row_at(q, y, base, own_rows, edge_base, edge_rows):
        if y < 0:
            return own_rows + edge_base + 2 * q + 1
        if y >= cells_y:
            return own_rows + (sides - 1) * edge_rows + edge_base + 2 * q
        return base + q * cells_y + y

    geo_rule = (0, geo_rows + rows, 0, 12)
    start_rule = (geo_rows, geo_rows + rows, 8, 12)
    field_rule = (0, rows, 0, 4)

    def inside(i):
        return [1, 2 - 2 * i] if cells_x == 2 else [1]

    def outside(i):
        return [2 * i] if cells_x == 2 else [0, 2]

    def in_block(j, k):
        return 0 <= j + k - 1 < cells_y

    def couple(i, j, dz, dx, k):
        cell = i * cells_y + j
        tile = first.at[dz, i + dx]

        def line(q):
            at = row_at(q, j + k - 1, *geo_rule)
            return tile[at : at + 1, :]

        bz = line(0) + (jnp.asarray(dz, jnp.int32) - 1).astype(jnp.float32)
        bx = line(1) + (jnp.asarray(dx, jnp.int32) - 1).astype(jnp.float32)
        by = line(2) + (k - 1.0)
        bs = line(3)
        for part in range(slots // CHUNK):
            span = pl.ds(part * CHUNK, CHUNK)
            ez = bz - local[cell, 0, span]
            ex = bx - local[cell, 1, span]
            ey = by - local[cell, 2, span]
            squared = ez * ez + ex * ex + ey * ey
            fraction = squared * lax.rsqrt(jnp.maximum(squared, 1e-30))
            reach = jnp.maximum(1.0 - fraction, 0.0)
            reach = reach * reach
            factor = coulomb_factor / cell_edge
            taper = reach * reach * (4.0 * factor * fraction + factor)
            pair[cell, (dz * 3 + dx) * 3 + k, span] = taper * lax.rsqrt(
                squared + (local[cell, 3, span] + bs)
            )

    def build():
        @pl.loop(0, cells_x)
        def _(i):
            for dx in inside(i):
                for j in range(cells_y):
                    for k in range(3):
                        if in_block(j, k):
                            couple(i, j, 1, dx, k)

        receive(*opening, layers=(0,))

        @pl.loop(0, cells_x)
        def _(i):
            for dx in outside(i):
                for j in range(cells_y):
                    for k in range(3):
                        couple(i, j, 1, dx, k)
            for dx in inside(i):
                for j in range(cells_y):
                    for k in range(3):
                        if not in_block(j, k):
                            couple(i, j, 1, dx, k)

        receive(*opening, layers=(1, -1))

        @pl.loop(0, cells_x)
        def _(i):
            @pl.loop(0, 6)
            def _(plane):
                dz, dx = 2 * (plane // 3), plane % 3
                for j in range(cells_y):
                    for k in range(3):
                        couple(i, j, dz, dx, k)

    def add_pairs(buffer, rule, i, j, total, planes, chosen):
        for dz, dx in planes:
            for k in range(3):
                if not chosen(dz, dx, k):
                    continue
                tile = buffer.at[dz, i + dx]
                block = pair[i * cells_y + j, (dz * 3 + dx) * 3 + k]
                for s in range(2):
                    at = row_at(s, j + k - 1, *rule)
                    total[s] = total[s] + block * tile[at : at + 1, :]
        return total

    def operate_own(buffer, rule):
        @pl.loop(0, cells_x)
        def _(i):
            for j in range(cells_y):
                total = [jnp.zeros(shape, jnp.float32) for _ in range(2)]
                total = add_pairs(
                    buffer, rule, i, j, total,
                    [(1, dx) for dx in inside(i)], lambda dz, dx, k: in_block(j, k),
                )
                for s in range(2):
                    sums[i, s * cells_y + j] = total[s]

    def operate_rest(buffer, rule, field):
        @pl.loop(0, cells_x)
        def _(i):
            for j in range(cells_y):
                total = [sums[i, s * cells_y + j] for s in range(2)]
                total = add_pairs(
                    buffer, rule, i, j, total,
                    [(1, dx) for dx in inside(i)], lambda dz, dx, k: not in_block(j, k),
                )
                total = add_pairs(
                    buffer, rule, i, j, total,
                    [(1, dx) for dx in outside(i)]
                    + [(dz, dx) for dz in (0, 2) for dx in range(3)],
                    lambda dz, dx, k: True,
                )
                for s in range(2):
                    sums[i, s * cells_y + j] = total[s]

        out = []
        for i in range(cells_x):
            lines = []
            for row in range(rows):
                column = jnp.sum(sums[i, row], axis=1, keepdims=True)
                lines.append(jnp.sum(jnp.where(eye, column, 0.0), axis=0, keepdims=True))
            out.append(occ[i] * (stiff[i] * field[i] + jnp.concatenate(lines, axis=0)))
        return out

    tile_shape = (rows, slots)
    lane = lax.broadcasted_iota(jnp.int32, tile_shape, 1)
    second = lax.broadcasted_iota(jnp.int32, tile_shape, 0) >= cells_y
    slot_of = lane - jnp.where(second, 8, 0)

    def part_copy(stage, peer, slot):
        return pltpu.make_async_remote_copy(
            src_ref=mine.at[stage],
            dst_ref=parts.at[stage, slot],
            send_sem=part_send.at[stage],
            recv_sem=part_recv.at[stage],
            device_id=peer,
            device_id_type=MESH,
        )

    def start_sums(stage, quantities):
        packed = jnp.zeros(tile_shape, jnp.float32)
        for k, quantity in enumerate(quantities):
            column = jnp.sum(functools.reduce(jnp.add, quantity), axis=1, keepdims=True)
            packed = jnp.where(slot_of == k, column, packed)
        mine[stage] = jnp.sum(packed, axis=0, keepdims=True)
        each_peer(lambda peer, slot: part_copy(stage, peer, slot).start())

    def finish_sums(stage, count):
        everything = parts.at[stage]
        pltpu.make_async_copy(everything, everything, part_recv.at[stage]).wait()
        row = mine[stage] + jnp.sum(parts[stage], axis=0)
        pltpu.make_async_copy(everything, everything, part_send.at[stage]).wait()
        return [
            jnp.where(
                second,
                jnp.broadcast_to(row[:, 8 + k : 9 + k], tile_shape),
                jnp.broadcast_to(row[:, k : k + 1], tile_shape),
            )
            for k in range(count)
        ]

    span = range(cells_x)

    def exchange_and_operate(stage, field, meanwhile=None):
        buffer, edge = fields.at[stage - 1], edges.at[stage - 1]
        for i in span:
            buffer[1, i + 1, :rows] = field[i]
            pieces = [field[i][:cells_y], field[i][cells_y:]]
            edge[i] = jnp.concatenate([end for v in pieces for end in ends(v)], axis=0)
        what = (stage, buffer, edge, rows)
        send(*what)
        if meanwhile is not None:
            meanwhile()
        operate_own(buffer, field_rule)
        receive(*what)
        out = operate_rest(buffer, field_rule, field)
        sent(*what)
        return out

    build()
    operate_own(first, start_rule)
    image = operate_rest(first, start_rule, x)
    sent(*opening)
    r = [rhs[i] - image[i] for i in span]
    w = exchange_and_operate(1, r)

    p = s = z = None
    for stage in range(ITERS):
        quantities = [[r[i] * r[i] for i in span], [w[i] * r[i] for i in span]]
        last = stage == ITERS - 1
        if last:
            quantities += [x, r, p]
        go = functools.partial(start_sums, stage, quantities)
        n = go() if last else exchange_and_operate(stage + 2, w, go)
        found = finish_sums(stage, len(quantities))
        gamma, delta = found[:2]
        if stage == 0:
            beta = None
            alpha = gamma / delta
            p, s, z = r, w, n
        else:
            beta = gamma / gamma_before
            alpha = gamma / (delta - beta * gamma / alpha)
            p = [r[i] + beta * p[i] for i in span]
            s = [w[i] + beta * s[i] for i in span]
            if not last:
                z = [n[i] + beta * z[i] for i in span]
        gamma_before = gamma
        x = [x[i] + alpha * p[i] for i in span]
        r = [r[i] - alpha * s[i] for i in span]
        if not last:
            w = [w[i] - alpha * z[i] for i in span]
    totals = found[2] + alpha * (found[3] + beta * found[4])
    ratio = totals[:cells_y] / totals[cells_y:]
    for i in span:
        charges[0, i] = x[i][:cells_y] - ratio * x[i][cells_y:]
        residuals[0, 0, i] = r[i][:cells_y]
        residuals[1, 0, i] = r[i][cells_y:]


def per_device(sizes, *arrays):
    type_ids = arrays[1]
    cells_x, cells_y, slots = type_ids.shape[1:]
    cells = cells_x * cells_y
    rows = 2 * cells_y
    devices = sizes[0] * sizes[1] * sizes[2]
    dys = (0, 1) if sizes[2] == 2 else (0, 1, -1)
    messages = 9 * len(dys) - 1
    halo = (3, cells_x + 2)
    sides = len(dys) - 1
    vmem = pl.BlockSpec(memory_space=pltpu.VMEM)
    return pl.pallas_call(
        functools.partial(kernel, sizes, dys),
        out_shape=(
            jax.ShapeDtypeStruct(type_ids.shape, jnp.float32),
            jax.ShapeDtypeStruct((2,) + type_ids.shape, jnp.float32),
        ),
        in_specs=[pl.BlockSpec(memory_space=pltpu.HBM)] * 7,
        out_specs=(vmem, vmem),
        scratch_shapes=[
            *(pltpu.VMEM(array.shape, array.dtype) for array in arrays[:4]),
            *(pltpu.SMEM(array.shape, array.dtype) for array in arrays[4:]),
            pltpu.VMEM(halo + (6 * cells_y + 12 * sides, slots), jnp.float32),
            pltpu.VMEM((ITERS,) + halo + (rows + 4 * sides, slots), jnp.float32),
            pltpu.VMEM((cells_x, 12, slots), jnp.float32),
            pltpu.VMEM((ITERS, cells_x, 4, slots), jnp.float32),
            pltpu.VMEM((cells, 27, slots, slots), jnp.float32),
            pltpu.VMEM((cells, 4, slots, slots), jnp.float32),
            pltpu.VMEM((cells_x, rows, slots, slots), jnp.float32),
            pltpu.VMEM((ITERS, devices - 1, 1, slots), jnp.float32),
            pltpu.VMEM((ITERS, 1, slots), jnp.float32),
            pltpu.SemaphoreType.DMA((len(arrays),)),
            pltpu.SemaphoreType.DMA((ITERS + 1, messages)),
            pltpu.SemaphoreType.DMA((ITERS + 1, messages)),
            pltpu.SemaphoreType.DMA((ITERS,)),
            pltpu.SemaphoreType.DMA((ITERS,)),
        ],
        compiler_params=pltpu.CompilerParams(
            collective_id=0, has_side_effects=True, vmem_limit_bytes=48 * 1024 * 1024
        ),
    )(*arrays)


def solution(mesh):
    sizes = tuple(mesh.shape[name] for name in AXES)
    in_specs = (
        P(None, "gz", "gx", "gy", None),
        P("gz", "gx", "gy", None),
        P("gz", "gx", "gy", None),
        P(None, "gz", "gx", "gy", None),
        P(),
        P(),
        P(),
    )
    out_specs = (P("gz", "gx", "gy", None), P(None, "gz", "gx", "gy", None))
    return jax.shard_map(
        functools.partial(per_device, sizes),
        mesh=mesh,
        in_specs=in_specs,
        out_specs=out_specs,
        check_vma=False,
    )
```

```python
import functools

import jax
import jax.numpy as jnp
from jax import lax
from jax.experimental import pallas as pl
from jax.experimental.pallas import tpu as pltpu
from jax.sharding import PartitionSpec as P

ITERS = 4
AXES = ("gz", "gx", "gy")
MESH = pl.DeviceIdType.MESH

coulomb_factor = 14.4
cell_edge = 10.0
CHUNK = 64


def kernel(
    sizes, dys,
    offsets_in, type_ids_in, occupied_in, prior_in, electro_in, hardness_in, shielding_in,
    charges, residuals,
    offsets, type_ids, occupied, prior, electro, hardness, shielding,
    first, fields, first_edge, edges, pair, local, sums, parts, mine,
    in_sem, send_sem, recv_sem, part_send, part_recv,
):
    loads = [
        pltpu.make_async_copy(source, target, in_sem.at[k])
        for k, (source, target) in enumerate(
            zip(
                (offsets_in, type_ids_in, occupied_in, prior_in,
                 electro_in, hardness_in, shielding_in),
                (offsets, type_ids, occupied, prior, electro, hardness, shielding),
            )
        )
    ]
    for load in loads:
        load.start()
    nz, nx, ny = sizes
    cells_x, cells_y, slots = type_ids.shape[1:]
    rows = 2 * cells_y
    geo_rows = 4 * cells_y
    cells = cells_x * cells_y
    devices = nz * nx * ny
    sides = len(dys) - 1
    me_z, me_x, me_y = (lax.axis_index(name) for name in AXES)

    at_x = [lax.rem(me_x + d, nx) for d in range(nx)]
    at_y = [lax.rem(me_y + d, ny) for d in range(ny)]

    def each_peer(action):
        def layer(dz, skip):
            z = lax.rem(me_z + dz, nz)
            for dx in range(nx):
                for dy in range(ny):
                    if not (skip and dx == 0 and dy == 0):
                        action((z, at_x[dx], at_y[dy]), (dz * nx + dx) * ny + dy - 1)

        layer(0, True)
        if nz <= 4:
            for dz in range(1, nz):
                layer(dz, False)
        else:
            pl.loop(1, nz)(lambda dz: layer(dz, False))

    barrier = pltpu.get_barrier_semaphore()
    each_peer(
        lambda peer, slot: pl.semaphore_signal(
            barrier, inc=1, device_id=peer, device_id_type=MESH
        )
    )

    def per_atom(table, ids):
        summed = jnp.zeros(ids.shape, jnp.float32)
        for species in range(table.shape[0]):
            summed = summed + jnp.where(ids == species, table[species], 0.0)
        return summed

    for load in loads:
        load.wait()
    occ, stiff, rhs, x = [], [], [], []

    def ends(values):
        return [values[:1], values[cells_y - 1 : cells_y]]

    for i in range(cells_x):
        ids = type_ids[0, i]
        occ_i = occupied[0, i].astype(jnp.float32)
        radius = per_atom(shielding, ids) * (1.0 / cell_edge)
        geo = [offsets[c, 0, i] * (1.0 / cell_edge) for c in range(3)] + [radius * radius]
        first[1, i + 1, :geo_rows] = jnp.concatenate(geo, axis=0)
        stiff_i = per_atom(hardness, ids)
        affinity = per_atom(electro, ids)
        occ.append(jnp.concatenate([occ_i, occ_i], axis=0))
        stiff.append(jnp.concatenate([stiff_i, stiff_i], axis=0))
        rhs.append(jnp.concatenate([-affinity * occ_i, -occ_i], axis=0))
        start = jnp.concatenate([prior[0, 0, i] * occ_i, prior[1, 0, i] * occ_i], axis=0)
        x.append(start)
        first[1, i + 1, geo_rows : geo_rows + rows] = start
        pieces = geo + [start[:cells_y], start[cells_y:]]
        first_edge[i] = jnp.concatenate([end for v in pieces for end in ends(v)], axis=0)

    for edge, slot in ((0, 0), (nz - 1, 2)):

        @pl.when(me_z == edge)
        def _():
            first[slot] = jnp.zeros(first.shape[1:], jnp.float32)
            for k in range(ITERS):
                fields[k, slot] = jnp.zeros(fields.shape[2:], jnp.float32)

    messages = [
        (dz, dx, dy)
        for dz in (1, -1, 0)
        for dx in (1, -1, 0)
        for dy in reversed(dys)
        if (dz, dx, dy) != (0, 0, 0)
    ]
    turn_x = {d: lax.rem(me_x + d + nx, nx) for d in (0, 1, -1)}
    turn_y = {d: lax.rem(me_y + d + ny, ny) for d in (0, 1, -1)}

    def copies(stage, buffer, edge, own_rows, action, layers=(1, -1, 0)):
        edge_rows = edge.shape[1]
        for m, (dz, dx, dy) in enumerate(messages):
            if dz not in layers:
                continue
            source, target, count = {
                0: (0, 1, cells_x),
                1: (cells_x - 1, 0, 1),
                -1: (0, cells_x + 1, 1),
            }[dx]
            if dy == 0:
                src = buffer.at[1, pl.ds(source + 1, count), pl.ds(0, own_rows)]
                span = pl.ds(0, own_rows)
            else:
                src = edge.at[pl.ds(source, count)]
                span = pl.ds(own_rows + (dys.index(dy) - 1) * edge_rows, edge_rows)
            copy = pltpu.make_async_remote_copy(
                src_ref=src,
                dst_ref=buffer.at[1 - dz, pl.ds(target, count), span],
                send_sem=send_sem.at[stage, m],
                recv_sem=recv_sem.at[stage, m],
                device_id=(me_z + dz, turn_x[dx], turn_y[dy]),
                device_id_type=MESH,
            )
            action(copy, dz)

    def guarded(name, sign):
        def go(copy, dz):
            act = getattr(copy, name)
            if dz == 0:
                act()
            else:
                other = me_z + sign * dz
                pl.when((other >= 0) & (other < nz))(act)

        return go

    def send(*what):
        copies(*what, guarded("start", 1))

    def receive(*what, layers=(1, -1, 0)):
        copies(*what, guarded("wait_recv", -1), layers)

    def sent(*what):
        copies(*what, guarded("wait_send", 1))

    opening = (0, first, first_edge, geo_rows + rows)
    pl.semaphore_wait(barrier, devices - 1)
    send(*opening)

    shape = (slots, slots)
    eye = lax.broadcasted_iota(jnp.int32, shape, 0) == lax.broadcasted_iota(jnp.int32, shape, 1)

    @pl.loop(0, cells)
    def _(cell):
        i, j = cell // cells_y, cell % cells_y
        for c in range(4):
            row = first[1, i + 1, pl.ds(c * cells_y + j, 1), :]
            column = jnp.sum(jnp.where(eye, row, 0.0), axis=1, keepdims=True)
            local[cell, c] = jnp.broadcast_to(column, shape)

    def row_at(q, y, base, own_rows, edge_base, edge_rows):
        if y < 0:
            return own_rows + edge_base + 2 * q + 1
        if y >= cells_y:
            return own_rows + (sides - 1) * edge_rows + edge_base + 2 * q
        return base + q * cells_y + y

    geo_rule = (0, geo_rows + rows, 0, 12)
    start_rule = (geo_rows, geo_rows + rows, 8, 12)
    field_rule = (0, rows, 0, 4)

    def inside(i):
        return [1, 2 - 2 * i] if cells_x == 2 else [1]

    def outside(i):
        return [2 * i] if cells_x == 2 else [0, 2]

    def in_block(j, k):
        return 0 <= j + k - 1 < cells_y

    def couple(i, j, dz, dx, k):
        cell = i * cells_y + j
        tile = first.at[dz, i + dx]

        def line(q):
            at = row_at(q, j + k - 1, *geo_rule)
            return tile[at : at + 1, :]

        bz = line(0) + (jnp.asarray(dz, jnp.int32) - 1).astype(jnp.float32)
        bx = line(1) + (jnp.asarray(dx, jnp.int32) - 1).astype(jnp.float32)
        by = line(2) + (k - 1.0)
        bs = line(3)
        for part in range(slots // CHUNK):
            span = pl.ds(part * CHUNK, CHUNK)
            ez = bz - local[cell, 0, span]
            ex = bx - local[cell, 1, span]
            ey = by - local[cell, 2, span]
            squared = ez * ez + ex * ex + ey * ey
            fraction = squared * lax.rsqrt(jnp.maximum(squared, 1e-30))
            reach = jnp.maximum(1.0 - fraction, 0.0)
            reach = reach * reach
            factor = coulomb_factor / cell_edge
            taper = reach * reach * (4.0 * factor * fraction + factor)
            pair[cell, (dz * 3 + dx) * 3 + k, span] = taper * lax.rsqrt(
                squared + (local[cell, 3, span] + bs)
            )

    def build():
        @pl.loop(0, cells_x)
        def _(i):
            for dx in inside(i):
                for j in range(cells_y):
                    for k in range(3):
                        if in_block(j, k):
                            couple(i, j, 1, dx, k)

        receive(*opening, layers=(0,))

        @pl.loop(0, cells_x)
        def _(i):
            for dx in outside(i):
                for j in range(cells_y):
                    for k in range(3):
                        couple(i, j, 1, dx, k)
            for dx in inside(i):
                for j in range(cells_y):
                    for k in range(3):
                        if not in_block(j, k):
                            couple(i, j, 1, dx, k)

        receive(*opening, layers=(1, -1))

        @pl.loop(0, cells_x)
        def _(i):
            @pl.loop(0, 6)
            def _(plane):
                dz, dx = 2 * (plane // 3), plane % 3
                for j in range(cells_y):
                    for k in range(3):
                        couple(i, j, dz, dx, k)

    def add_pairs(buffer, rule, i, j, total, planes, chosen):
        for dz, dx in planes:
            for k in range(3):
                if not chosen(dz, dx, k):
                    continue
                tile = buffer.at[dz, i + dx]
                block = pair[i * cells_y + j, (dz * 3 + dx) * 3 + k]
                for s in range(2):
                    at = row_at(s, j + k - 1, *rule)
                    total[s] = total[s] + block * tile[at : at + 1, :]
        return total

    def operate_own(buffer, rule):
        @pl.loop(0, cells_x)
        def _(i):
            for j in range(cells_y):
                total = [jnp.zeros(shape, jnp.float32) for _ in range(2)]
                total = add_pairs(
                    buffer, rule, i, j, total,
                    [(1, dx) for dx in inside(i)], lambda dz, dx, k: in_block(j, k),
                )
                for s in range(2):
                    sums[i, s * cells_y + j] = total[s]

    def operate_rest(buffer, rule, field):
        @pl.loop(0, cells_x)
        def _(i):
            for j in range(cells_y):
                total = [sums[i, s * cells_y + j] for s in range(2)]
                total = add_pairs(
                    buffer, rule, i, j, total,
                    [(1, dx) for dx in inside(i)], lambda dz, dx, k: not in_block(j, k),
                )
                total = add_pairs(
                    buffer, rule, i, j, total,
                    [(1, dx) for dx in outside(i)]
                    + [(dz, dx) for dz in (0, 2) for dx in range(3)],
                    lambda dz, dx, k: True,
                )
                for s in range(2):
                    sums[i, s * cells_y + j] = total[s]

        out = []
        for i in range(cells_x):
            lines = []
            for row in range(rows):
                column = jnp.sum(sums[i, row], axis=1, keepdims=True)
                lines.append(jnp.sum(jnp.where(eye, column, 0.0), axis=0, keepdims=True))
            out.append(occ[i] * (stiff[i] * field[i] + jnp.concatenate(lines, axis=0)))
        return out

    tile_shape = (rows, slots)
    lane = lax.broadcasted_iota(jnp.int32, tile_shape, 1)
    second = lax.broadcasted_iota(jnp.int32, tile_shape, 0) >= cells_y
    slot_of = lane - jnp.where(second, 8, 0)

    def part_copy(stage, peer, slot):
        return pltpu.make_async_remote_copy(
            src_ref=mine.at[stage],
            dst_ref=parts.at[stage, slot],
            send_sem=part_send.at[stage],
            recv_sem=part_recv.at[stage],
            device_id=peer,
            device_id_type=MESH,
        )

    def start_sums(stage, quantities):
        packed = jnp.zeros(tile_shape, jnp.float32)
        for k, quantity in enumerate(quantities):
            column = jnp.sum(functools.reduce(jnp.add, quantity), axis=1, keepdims=True)
            packed = jnp.where(slot_of == k, column, packed)
        mine[stage] = jnp.sum(packed, axis=0, keepdims=True)
        each_peer(lambda peer, slot: part_copy(stage, peer, slot).start())

    def finish_sums(stage, count):
        everything = parts.at[stage]
        pltpu.make_async_copy(everything, everything, part_recv.at[stage]).wait()
        row = mine[stage] + jnp.sum(parts[stage], axis=0)
        pltpu.make_async_copy(everything, everything, part_send.at[stage]).wait()
        return [
            jnp.where(
                second,
                jnp.broadcast_to(row[:, 8 + k : 9 + k], tile_shape),
                jnp.broadcast_to(row[:, k : k + 1], tile_shape),
            )
            for k in range(count)
        ]

    span = range(cells_x)

    def exchange_and_operate(stage, field, meanwhile=None):
        buffer, edge = fields.at[stage - 1], edges.at[stage - 1]
        for i in span:
            buffer[1, i + 1, :rows] = field[i]
            pieces = [field[i][:cells_y], field[i][cells_y:]]
            edge[i] = jnp.concatenate([end for v in pieces for end in ends(v)], axis=0)
        what = (stage, buffer, edge, rows)
        send(*what)
        if meanwhile is not None:
            meanwhile()
        operate_own(buffer, field_rule)
        receive(*what)
        out = operate_rest(buffer, field_rule, field)
        sent(*what)
        return out

    build()
    operate_own(first, start_rule)
    image = operate_rest(first, start_rule, x)
    sent(*opening)
    r = [rhs[i] - image[i] for i in span]
    w = exchange_and_operate(1, r)

    p = s = z = None
    for stage in range(ITERS):
        quantities = [[r[i] * r[i] for i in span], [w[i] * r[i] for i in span]]
        last = stage == ITERS - 1
        if last:
            quantities += [x, r, p]
        go = functools.partial(start_sums, stage, quantities)
        n = go() if last else exchange_and_operate(stage + 2, w, go)
        found = finish_sums(stage, len(quantities))
        gamma, delta = found[:2]
        if stage == 0:
            beta = None
            alpha = gamma / delta
            p, s, z = r, w, n
        else:
            beta = gamma / gamma_before
            alpha = gamma / (delta - beta * gamma / alpha)
            p = [r[i] + beta * p[i] for i in span]
            s = [w[i] + beta * s[i] for i in span]
            if not last:
                z = [n[i] + beta * z[i] for i in span]
        gamma_before = gamma
        x = [x[i] + alpha * p[i] for i in span]
        r = [r[i] - alpha * s[i] for i in span]
        if not last:
            w = [w[i] - alpha * z[i] for i in span]
    totals = found[2] + alpha * (found[3] + beta * found[4])
    ratio = totals[:cells_y] / totals[cells_y:]
    for i in span:
        charges[0, i] = x[i][:cells_y] - ratio * x[i][cells_y:]
        residuals[0, 0, i] = r[i][:cells_y]
        residuals[1, 0, i] = r[i][cells_y:]


def per_device(sizes, *arrays):
    type_ids = arrays[1]
    cells_x, cells_y, slots = type_ids.shape[1:]
    cells = cells_x * cells_y
    rows = 2 * cells_y
    devices = sizes[0] * sizes[1] * sizes[2]
    dys = (0, 1) if sizes[2] == 2 else (0, 1, -1)
    messages = 9 * len(dys) - 1
    halo = (3, cells_x + 2)
    sides = len(dys) - 1
    vmem = pl.BlockSpec(memory_space=pltpu.VMEM)
    return pl.pallas_call(
        functools.partial(kernel, sizes, dys),
        out_shape=(
            jax.ShapeDtypeStruct(type_ids.shape, jnp.float32),
            jax.ShapeDtypeStruct((2,) + type_ids.shape, jnp.float32),
        ),
        in_specs=[pl.BlockSpec(memory_space=pl.ANY)] * 7,
        out_specs=(vmem, vmem),
        scratch_shapes=[
            *(pltpu.VMEM(array.shape, array.dtype) for array in arrays[:4]),
            *(pltpu.SMEM(array.shape, array.dtype) for array in arrays[4:]),
            pltpu.VMEM(halo + (6 * cells_y + 12 * sides, slots), jnp.float32),
            pltpu.VMEM((ITERS,) + halo + (rows + 4 * sides, slots), jnp.float32),
            pltpu.VMEM((cells_x, 12, slots), jnp.float32),
            pltpu.VMEM((ITERS, cells_x, 4, slots), jnp.float32),
            pltpu.VMEM((cells, 27, slots, slots), jnp.float32),
            pltpu.VMEM((cells, 4, slots, slots), jnp.float32),
            pltpu.VMEM((cells_x, rows, slots, slots), jnp.float32),
            pltpu.VMEM((ITERS, devices - 1, 1, slots), jnp.float32),
            pltpu.VMEM((ITERS, 1, slots), jnp.float32),
            pltpu.SemaphoreType.DMA((len(arrays),)),
            pltpu.SemaphoreType.DMA((ITERS + 1, messages)),
            pltpu.SemaphoreType.DMA((ITERS + 1, messages)),
            pltpu.SemaphoreType.DMA((ITERS,)),
            pltpu.SemaphoreType.DMA((ITERS,)),
        ],
        compiler_params=pltpu.CompilerParams(
            collective_id=0, has_side_effects=True, vmem_limit_bytes=60 * 1024 * 1024
        ),
    )(*arrays)


def solution(mesh):
    sizes = tuple(mesh.shape[name] for name in AXES)
    in_specs = (
        P(None, "gz", "gx", "gy", None),
        P("gz", "gx", "gy", None),
        P("gz", "gx", "gy", None),
        P(None, "gz", "gx", "gy", None),
        P(),
        P(),
        P(),
    )
    out_specs = (P("gz", "gx", "gy", None), P(None, "gz", "gx", "gy", None))
    return jax.shard_map(
        functools.partial(per_device, sizes),
        mesh=mesh,
        in_specs=in_specs,
        out_specs=out_specs,
        check_vma=False,
    )
```
